32 devices in a mesh: groups: 2 (over y), vocab: 16 (over z, x, core).
Axes of the slice: x: 2, y: 2, z: 4, core: 2. Of those that a mesh axis runs over, the one named last changes fastest.
Arguments:
- hidden: bfloat16 [512, 1280], P(('groups', 'vocab')), parts along dimension 0, may hold values from -320 to 320
- embedding: bfloat16 [6144, 1280], P('vocab'), may hold values from -0.15625 to 0.15625
- prev_tokens: int32 [2, 512], P(None, 'groups'), parts along dimension 1, may hold values from 0 to 6143, as said below
- last_stamp: int32 [512], P('groups'), parts along dimension 0, may hold values from -1 to 1500, as said below
- sample_begin: int32 [512], P('groups'), parts along dimension 0, may hold values from 1 to 4
- seq_length: int32 [512], P('groups'), parts along dimension 0, may hold values from 1 to 9, as said below
- chosen: int32 [5, 512], P(None, 'groups'), parts along dimension 1, may hold values from 0 to 6143
Outputs:
- picked_logprob: float32 [5, 512], P(None, ('groups', 'vocab')), parts along dimension 1
- stamp_logprob: float32 [512], P(('groups', 'vocab')), parts along dimension 0
The draws below stay inside these ranges and needn't reach their ends.
There are 2 independent parts, one for each index of `groups`. The reference program is written for one: setup_inputs(seed, part) draws one part's arguments, and reference() takes and returns one part's arrays. A program takes and returns all parts, laid end to end along the dimension named above; an argument that names none is the same for every part. Nothing has to cross between parts.
Inputs may be any that keep to these rules, and one draw needn't show every extreme that they name: prev_tokens[1, r] is row r's latest token and prev_tokens[0, r] the one before; ids at or above 4643 are timestamps. `last_stamp`: index among the 1501 timestamps of the latest timestamp token sampled since the row's sample begin, -1 if none; equal to the latest token's index when that token is a timestamp and was sampled. `seq_length`: at least the row's sample_begin and at most sample_begin + 5.
All inputs are finite; a program needn't handle non-finite values.
Results may differ from the reference program's by a relative error of at most 0.0003.
Values may be sent and summed in bfloat16 or wider, within the bound.
No kernel may reach another device: no remote copies, remote signals or barrier semaphores. Data moves between devices by JAX's collectives and lax.ppermute only.
A program may use at most 64 MiB of HBM per device.

```python
import math
import jax
import jax.numpy as jnp
from jax import lax

D = 1280
VOCAB = 6144
TSN = 1501
SPECIALS = 108
INITIAL = 50
NSEL = 5
ROWS = 256


def history(key):
    keys = jax.random.split(jax.random.fold_in(key, 4242), 8)
    stamp_begin = VOCAB - TSN
    begin = jax.random.randint(keys[0], (ROWS,), 1, 5)
    generated = jax.random.randint(keys[1], (ROWS,), 0, 6)
    last_flag = jax.random.randint(keys[2], (ROWS,), 0, 2) == 1
    before_flag = jax.random.randint(keys[3], (ROWS,), 0, 2) == 1
    last_index = jax.random.randint(keys[4], (ROWS,), 0, TSN)
    before_index = jax.random.randint(keys[5], (ROWS,), 0, TSN)
    text_tokens = jax.random.randint(keys[6], (2, ROWS), 0, stamp_begin - SPECIALS)
    earlier = jnp.maximum(jax.random.randint(keys[7], (ROWS,), -TSN, TSN), -1)
    last_is = last_flag & (generated >= 1)
    before_is = before_flag & (generated >= 2)
    last_token = jnp.where(last_is, stamp_begin + last_index, text_tokens[1])
    before_token = jnp.where(before_is, stamp_begin + before_index, text_tokens[0])
    stamp = jnp.where(last_is, last_index, jnp.where(before_is, before_index, jnp.where(generated >= 3, earlier, -1)))
    tokens = jnp.stack([before_token, last_token]).astype(jnp.int32)
    return (tokens, stamp.astype(jnp.int32), begin.astype(jnp.int32), (begin + generated).astype(jnp.int32))


def draw_prev_tokens(key, part):
    return history(key)[0]


def draw_last_stamp(key, part):
    return history(key)[1]


def draw_sample_begin(key, part):
    return history(key)[2]


def draw_seq_length(key, part):
    return history(key)[3]


def draw_hidden(key, part):
    first, second = jax.random.split(key)
    values = jnp.clip(3.0 * jax.random.normal(first, (ROWS, D), jnp.float32), -18.0, 18.0)
    return values.astype(jnp.bfloat16)


def touch_ends(drawn, rng, smallest, high):
    longest = drawn.shape.index(max(drawn.shape))
    spots = []
    for shift in (0, 1):
        where = [jax.random.randint(jax.random.fold_in(rng, axis), (), 0, length) for axis, length in enumerate(drawn.shape)]
        where[longest] = (where[longest] + shift) % drawn.shape[longest]
        spots.append(tuple(where))
    return drawn.at[spots[0]].set(smallest).at[spots[1]].set(high)


def block_levels(own_key, extent, pieces, smallest, high):
    def one(dim, shards_of):
        steps = jax.random.uniform(jax.random.fold_in(jax.random.fold_in(own_key, 6), dim), (shards_of,), jnp.float32, smallest / len(pieces), high / len(pieces))
        return jnp.repeat(jnp.exp(steps), extent[dim] // shards_of).reshape((-1,) + (1,) * (len(extent) - dim - 1))

    factor_of = one(*pieces[0])
    for cut in pieces[1:]:
        factor_of = factor_of * one(*cut)
    return factor_of


def bell_draw(rng, extent, width, most, shards=(), kind=jnp.bfloat16):
    gain = block_levels(rng, extent, shards, -0.22, 0.18) if shards else 1.0
    array = jax.random.normal(rng, extent, jnp.float32) * width * gain
    return jnp.minimum(jnp.maximum(array, -most), most).astype(kind)


def setup_inputs(seed: int = 0, part: int = 0) -> dict:
    streams_of = jax.random.split(jax.random.key(seed), 8)
    own_keys = jax.random.split(jax.random.fold_in(streams_of[7], part), 8)
    return {
        "hidden": draw_hidden(jax.random.fold_in(jax.random.fold_in(streams_of[7], part), 71), part),
        "embedding": bell_draw(streams_of[1], (VOCAB, D), D ** -0.5, 0.15625, ((0, 16),)),
        "prev_tokens": draw_prev_tokens(jax.random.fold_in(jax.random.fold_in(streams_of[7], part), 71), part),
        "last_stamp": draw_last_stamp(jax.random.fold_in(jax.random.fold_in(streams_of[7], part), 71), part),
        "sample_begin": draw_sample_begin(jax.random.fold_in(jax.random.fold_in(streams_of[7], part), 71), part),
        "seq_length": draw_seq_length(jax.random.fold_in(jax.random.fold_in(streams_of[7], part), 71), part),
        "chosen": touch_ends(jax.random.randint(own_keys[6], (NSEL, ROWS), 0, VOCAB), jax.random.fold_in(own_keys[6], 1), 0, VOCAB - 1).astype(jnp.int32),
    }


MASK_VALUE = -1.0e9
SLOPE = 4.0
FLOOR = -30.0


def rule_mask(columns, prev_tokens, last_stamp, sample_begin, seq_length, stamp_begin):
    generated = seq_length - sample_begin
    last_is = (generated >= 1) & (prev_tokens[1] >= stamp_begin)
    before_is = (generated < 2) | (prev_tokens[0] >= stamp_begin)
    column = columns[None, :]
    is_stamp = column >= stamp_begin
    offset = column - stamp_begin
    masked = column == stamp_begin - 1
    masked = masked | ((last_is & before_is)[:, None] & is_stamp)
    masked = masked | ((last_is & ~before_is)[:, None] & (column < stamp_begin - SPECIALS))
    bound = last_stamp + jnp.where(last_is & ~before_is, 0, 1).astype(jnp.int32)
    masked = masked | (is_stamp & (offset < bound[:, None]) & (last_stamp >= 0)[:, None])
    begin = (generated == 0)[:, None]
    masked = masked | (begin & (column < stamp_begin))
    masked = masked | (begin & is_stamp & (offset > INITIAL))
    return masked


def finalize(text_max, text_total, stamp_max, stamp_total, picked, chosen, stamp_begin):
    text_lse = text_max + jnp.log(text_total)
    stamp_lse = stamp_max + jnp.log(stamp_total)
    penalty = SLOPE * jnp.maximum(stamp_lse - text_max, 0.0)
    shifted = text_lse - penalty
    larger = jnp.maximum(shifted, stamp_lse)
    total = larger + jnp.log(jnp.exp(shifted - larger) + jnp.exp(stamp_lse - larger))
    adjusted = picked - jnp.where(chosen < stamp_begin, penalty[None, :], 0.0) - total[None, :]
    return jnp.maximum(adjusted, FLOOR), jnp.maximum(stamp_lse - total, FLOOR)


def reference(hidden, embedding, prev_tokens, last_stamp, sample_begin, seq_length, chosen):
    stamp_begin = VOCAB - TSN
    columns = jnp.arange(VOCAB, dtype=jnp.int32)
    is_text = columns < stamp_begin
    block = math.gcd(ROWS, 256)
    blocks = ROWS // block

    def one_block(index):
        start = (index * block).astype(jnp.int32)
        rows = lax.dynamic_slice_in_dim(hidden, start, block, 0)
        prev = lax.dynamic_slice_in_dim(prev_tokens, start, block, 1)
        stamp = lax.dynamic_slice_in_dim(last_stamp, start, block, 0)
        begin = lax.dynamic_slice_in_dim(sample_begin, start, block, 0)
        length = lax.dynamic_slice_in_dim(seq_length, start, block, 0)
        pick = lax.dynamic_slice_in_dim(chosen, start, block, 1)
        logits = lax.dot_general(rows, embedding, (((1,), (1,)), ((), ())), preferred_element_type=jnp.float32)
        masked = rule_mask(columns, prev, stamp, begin, length, stamp_begin)
        values = jnp.where(masked, MASK_VALUE, logits)
        text_max = jnp.max(jnp.where(is_text, values, -jnp.inf), axis=1)
        text_total = jnp.sum(jnp.where(is_text, jnp.exp(values - text_max[:, None]), 0.0), axis=1)
        stamp_max = jnp.max(jnp.where(is_text, -jnp.inf, values), axis=1)
        stamp_total = jnp.sum(jnp.where(is_text, 0.0, jnp.exp(values - stamp_max[:, None])), axis=1)
        picked = jnp.take_along_axis(values, pick.T, axis=1).T
        return text_max, text_total, stamp_max, stamp_total, picked

    text_max, text_total, stamp_max, stamp_total, picked = lax.map(one_block, jnp.arange(blocks, dtype=jnp.int32))
    picked = jnp.transpose(picked, (1, 0, 2)).reshape(NSEL, ROWS)
    return finalize(text_max.reshape(ROWS), text_total.reshape(ROWS), stamp_max.reshape(ROWS), stamp_total.reshape(ROWS), picked, chosen, stamp_begin)
```

```python
import jax
import jax.numpy as jnp
from jax import lax
from jax.sharding import PartitionSpec as P

TSN = 1501
SPECIALS = 108
INITIAL = 50

MASK_VALUE = -1000000000.0
EMPTY_VALUE = -3000000000.0
SLOPE = 4.0
FLOOR = -30.0


def rule_mask(column, prev_tokens, last_stamp, sample_begin, seq_length, stamp_begin):
    generated = seq_length - sample_begin
    last_is = (generated >= 1) & (prev_tokens[1] >= stamp_begin)
    before_is = (generated < 2) | (prev_tokens[0] >= stamp_begin)
    both = last_is & before_is
    single = last_is & ~before_is
    is_stamp = column >= stamp_begin
    offset = column - stamp_begin
    masked = column == stamp_begin - 1
    masked = masked | both[None, :] & is_stamp
    masked = masked | single[None, :] & (column < stamp_begin - SPECIALS)
    bound = last_stamp + jnp.where(single, 0, 1).astype(jnp.int32)
    masked = masked | is_stamp & (offset < bound[None, :]) & (last_stamp >= 0)[None, :]
    begin = (generated == 0)[None, :]
    masked = masked | begin & (column < stamp_begin)
    masked = masked | begin & (offset > INITIAL)
    return masked


def shard_stats(rows, table, first_column, prev, stamp, begin, length, chosen, stamp_begin):
    width = table.shape[0]
    logits = lax.dot_general(
        table, rows, (((1,), (1,)), ((), ())), preferred_element_type=jnp.float32
    )
    column = first_column + lax.broadcasted_iota(jnp.int32, (width, 1), 0)
    is_text = column < stamp_begin
    masked = rule_mask(column, prev, stamp, begin, length, stamp_begin)
    values = jnp.where(masked, MASK_VALUE, logits)
    text_max = jnp.max(jnp.where(is_text, values, EMPTY_VALUE), axis=0)
    stamp_max = jnp.max(jnp.where(is_text, EMPTY_VALUE, values), axis=0)
    scaled = jnp.exp(values - jnp.where(is_text, text_max[None, :], stamp_max[None, :]))
    text_total = jnp.sum(jnp.where(is_text, scaled, 0.0), axis=0)
    stamp_total = jnp.sum(jnp.where(is_text, 0.0, scaled), axis=0)
    picked = [
        jnp.sum(jnp.where(column == chosen[k][None, :], values, 0.0), axis=0)
        for k in range(chosen.shape[0])
    ]
    text_lse = text_max + jnp.log(text_total)
    stamp_lse = stamp_max + jnp.log(stamp_total)
    return jnp.stack([text_max, text_lse, stamp_lse] + picked)


def merged_lse(parts):
    top = jnp.max(parts, axis=0)
    return top + jnp.log(jnp.sum(jnp.exp(parts - top[None, :]), axis=0))


def finalize(stats, chosen, stamp_begin):
    text_max = jnp.max(stats[:, 0], axis=0)
    text_lse = merged_lse(stats[:, 1])
    stamp_lse = merged_lse(stats[:, 2])
    picked = jnp.sum(stats[:, 3:], axis=0)
    penalty = SLOPE * jnp.maximum(stamp_lse - text_max, 0.0)
    shifted = text_lse - penalty
    larger = jnp.maximum(shifted, stamp_lse)
    total = larger + jnp.log(jnp.exp(shifted - larger) + jnp.exp(stamp_lse - larger))
    adjusted = picked - jnp.where(chosen < stamp_begin, penalty[None, :], 0.0) - total[None, :]
    return (jnp.maximum(adjusted, FLOOR), jnp.maximum(stamp_lse - total, FLOOR))


def per_device(hidden, embedding, prev_tokens, last_stamp, sample_begin, seq_length, chosen):
    width = embedding.shape[0]
    row_dev = hidden.shape[0]
    count = lax.axis_size("vocab")
    index = lax.axis_index("vocab")
    stamp_begin = width * count - TSN
    rows = lax.all_gather(hidden, "vocab", axis=0, tiled=True)
    stats = shard_stats(
        rows, embedding, index * width, prev_tokens, last_stamp, sample_begin, seq_length,
        chosen, stamp_begin,
    )
    fields = stats.shape[0]
    sent = stats.reshape(fields, count, row_dev).transpose(1, 0, 2)
    got = lax.all_to_all(sent, "vocab", 0, 0, tiled=True)
    own_chosen = lax.dynamic_slice_in_dim(chosen, index * row_dev, row_dev, 1)
    return finalize(got, own_chosen, stamp_begin)


def solution(mesh):
    placed = (
        P(("groups", "vocab"), None),
        P("vocab", None),
        P(None, "groups"),
        P("groups"),
        P("groups"),
        P("groups"),
        P(None, "groups"),
    )
    return jax.shard_map(
        per_device,
        mesh=mesh,
        in_specs=placed,
        out_specs=(P(None, ("groups", "vocab")), P(("groups", "vocab"))),
        check_vma=False,
    )
```

```python
import functools

import jax
import jax.numpy as jnp
from jax import lax
from jax.experimental import pallas as pl
from jax.experimental.pallas import tpu as pltpu
from jax.sharding import PartitionSpec as P

TSN = 1501
SPECIALS = 108
INITIAL = 50

MASK_VALUE = -1000000000.0
EMPTY_VALUE = -3000000000.0
SLOPE = 4.0
FLOOR = -30.0


LANES = 128
FIELDS = 8
FAR = 1 << 30
GRANT = 24 << 20


def masks_of(outer):
    return [2 * k for k in range(outer)] + [2 * k + 1 for k in range(outer)]


def row_limits(prev_old, prev_new, last_stamp, sample_begin, seq_length, stamp_begin):
    generated = seq_length - sample_begin
    last_is = (generated >= 1) & (prev_new >= stamp_begin)
    before_is = (generated < 2) | (prev_old >= stamp_begin)
    both = last_is & before_is
    single = last_is & ~before_is
    begin = generated == 0
    text_low = jnp.where(begin, stamp_begin, jnp.where(single, stamp_begin - SPECIALS, 0))
    bound = stamp_begin + last_stamp + jnp.where(single, 0, 1)
    stamp_low = jnp.where(both, FAR, jnp.where(last_stamp >= 0, bound, stamp_begin))
    stamp_high = jnp.where(begin, stamp_begin + INITIAL + 1, FAR)
    return text_low, stamp_low, stamp_high


def prep_kernel(masks, row_dev, stamp_begin, prev, stamp, begin, length, chosen, out):
    index = lax.axis_index("vocab")
    per_tile = LANES // row_dev
    lane = lax.broadcasted_iota(jnp.int32, (FIELDS, LANES), 1)
    for tile in range(len(masks) // per_tile):
        total = jnp.zeros((FIELDS, LANES), jnp.int32)
        for place in range(per_tile):
            source = index ^ (2 * masks[tile * per_tile + place])
            at = pl.multiple_of(lax.div(source, per_tile) * LANES, LANES)
            span = pl.ds(at, LANES)
            limits = row_limits(
                prev[0:1, span], prev[1:2, span], stamp[:, span], begin[:, span], length[:, span],
                stamp_begin,
            )
            fields = jnp.concatenate(list(limits) + [chosen[:, span]], axis=0)
            shift = lax.rem(place - lax.rem(source, per_tile) + per_tile, per_tile) * row_dev
            moved = pltpu.roll(fields, shift, 1)
            here = (lane >= place * row_dev) & (lane < (place + 1) * row_dev)
            total = jnp.where(here, moved, total)
        out[:, tile * LANES:(tile + 1) * LANES] = total


def stats_kernel(masks, row_dev, stamp_begin, line, across, table, other, limits, out):
    index = lax.axis_index("vocab")
    member = lax.div(index, 2)
    width = table.shape[0]
    per_tile = LANES // row_dev
    pieces = jnp.concatenate([line[...], across[...]], axis=0)
    for tile in range(len(masks) // per_tile):
        span = slice(tile * LANES, (tile + 1) * LANES)
        rows = pieces[span]
        lim = limits[:, span]
        text_low, stamp_low, stamp_high = lim[0:1], lim[1:2], lim[2:3]
        halves = []
        for ref, shard in ((table, index), (other, index ^ 1)):
            logits = lax.dot_general(
                ref[...], rows, (((1,), (1,)), ((), ())), preferred_element_type=jnp.float32
            )
            column = shard * width + lax.broadcasted_iota(jnp.int32, (width, LANES), 0)
            is_text = column < stamp_begin
            low = jnp.where(is_text, text_low, stamp_low)
            high = jnp.where(is_text, stamp_begin - 1, stamp_high)
            values = jnp.where((column >= low) & (column < high), logits, MASK_VALUE)
            halves.append((values, column, is_text))
        text_max = stamp_max = None
        for values, column, is_text in halves:
            text = jnp.max(jnp.where(is_text, values, EMPTY_VALUE), axis=0, keepdims=True)
            stamp = jnp.max(jnp.where(is_text, EMPTY_VALUE, values), axis=0, keepdims=True)
            text_max = text if text_max is None else jnp.maximum(text_max, text)
            stamp_max = stamp if stamp_max is None else jnp.maximum(stamp_max, stamp)
        text_total = jnp.zeros((1, LANES), jnp.float32)
        stamp_total = jnp.zeros((1, LANES), jnp.float32)
        picked = [jnp.zeros((1, LANES), jnp.float32) for _ in range(FIELDS - 3)]
        for values, column, is_text in halves:
            scaled = jnp.exp(values - jnp.where(is_text, text_max, stamp_max))
            text_total += jnp.sum(jnp.where(is_text, scaled, 0.0), axis=0, keepdims=True)
            stamp_total += jnp.sum(jnp.where(is_text, 0.0, scaled), axis=0, keepdims=True)
            for k in range(FIELDS - 3):
                hit = column == lim[3 + k:4 + k]
                picked[k] += jnp.sum(jnp.where(hit, values, 0.0), axis=0, keepdims=True)
        stats = [text_max, text_max + jnp.log(text_total), stamp_max + jnp.log(stamp_total)] + picked
        lane = lax.broadcasted_iota(jnp.int32, (per_tile, LANES), 1)
        packed = jnp.zeros((per_tile, LANES), jnp.float32)
        stacked = jnp.concatenate([stats[(-f) % FIELDS] for f in range(FIELDS)], axis=0)
        turned = pltpu.roll(stacked, 0, 1, stride=row_dev, stride_axis=0)
        for f in range(FIELDS):
            spread = jnp.broadcast_to(turned[f:f + 1], (per_tile, LANES))
            moved = pltpu.roll(spread, 0, 1, stride=row_dev, stride_axis=0)
            here = (lane >= f * row_dev) & (lane < (f + 1) * row_dev)
            packed = jnp.where(here, moved, packed)
        for place in range(per_tile):
            target = member ^ masks[tile * per_tile + (-place) % per_tile]
            out[pl.ds(target, 1)] = packed[place:place + 1].reshape(1, 1, LANES)


def final_kernel(row_dev, stamp_begin, got, limits, picked_out, stamp_out):
    parts = got[:, 0, :]
    top = jnp.max(parts, axis=0, keepdims=True)
    lse = top + jnp.log(jnp.sum(jnp.exp(parts - top), axis=0, keepdims=True))
    total = jnp.sum(parts, axis=0, keepdims=True)
    lane = lax.broadcasted_iota(jnp.int32, (1, LANES), 1)
    lses = lane >= (FIELDS - 2) * row_dev
    merged = jnp.where(lane < row_dev, top, jnp.where(lses, lse, total))
    spread = jnp.broadcast_to(merged, (FIELDS, LANES))
    fields = pltpu.roll(spread, 0, 1, stride=row_dev, stride_axis=0)
    text_max, text_lse, stamp_lse = fields[0:1], fields[1:2], fields[2:3]
    penalty = SLOPE * jnp.maximum(stamp_lse - text_max, 0.0)
    shifted = text_lse - penalty
    larger = jnp.maximum(shifted, stamp_lse)
    total = larger + jnp.log(jnp.exp(shifted - larger) + jnp.exp(stamp_lse - larger))
    chosen = limits[:, 0:LANES]
    adjusted = fields - jnp.where(chosen < stamp_begin, penalty, 0.0) - total
    result = jnp.maximum(adjusted, FLOOR)
    picked_out[...] = result[3:, :row_dev]
    stamp_out[...] = jnp.maximum(stamp_lse - total, FLOOR)[:, :row_dev]


def per_device(hidden, embedding, prev_tokens, last_stamp, sample_begin, seq_length, chosen):
    width = embedding.shape[0]
    row_dev = hidden.shape[0]
    nsel = chosen.shape[0]
    count = lax.axis_size("vocab")
    members = count // 2
    outer = members // 2
    stamp_begin = width * count - TSN
    masks = masks_of(outer)
    core_rows = members * row_dev

    def swap(array, mask):
        return lax.ppermute(array, "vocab", [(i, i ^ mask) for i in range(count)])

    other = swap(embedding, 1)
    limits = pl.pallas_call(
        functools.partial(prep_kernel, masks, row_dev, stamp_begin),
        out_shape=jax.ShapeDtypeStruct((FIELDS, core_rows), jnp.int32),
        name="prep",
        compiler_params=pltpu.CompilerParams(vmem_limit_bytes=GRANT),
    )(prev_tokens, last_stamp[None], sample_begin[None], seq_length[None], chosen)
    line = jnp.concatenate([hidden] + [swap(hidden, 4 * k) for k in range(1, outer)], axis=0)
    across = swap(line, 2)
    stats = pl.pallas_call(
        functools.partial(stats_kernel, masks, row_dev, stamp_begin),
        out_shape=jax.ShapeDtypeStruct((members, 1, LANES), jnp.float32),
        name="stats",
        compiler_params=pltpu.CompilerParams(vmem_limit_bytes=GRANT),
    )(line, across, embedding, other, limits)
    same_core = [[2 * i + core for i in range(members)] for core in range(2)]
    got = lax.all_to_all(stats, "vocab", 0, 0, axis_index_groups=same_core, tiled=True)
    picked, stamped = pl.pallas_call(
        functools.partial(final_kernel, row_dev, stamp_begin),
        out_shape=(
            jax.ShapeDtypeStruct((nsel, row_dev), jnp.float32),
            jax.ShapeDtypeStruct((1, row_dev), jnp.float32),
        ),
        name="final",
        compiler_params=pltpu.CompilerParams(vmem_limit_bytes=GRANT),
    )(got, limits)
    return picked, stamped[0]


def solution(mesh):
    placed = (
        P(("groups", "vocab"), None),
        P("vocab", None),
        P(None, "groups"),
        P("groups"),
        P("groups"),
        P("groups"),
        P(None, "groups"),
    )
    return jax.shard_map(
        per_device,
        mesh=mesh,
        in_specs=placed,
        out_specs=(P(None, ("groups", "vocab")), P(("groups", "vocab"))),
        check_vma=False,
    )
```

```python
import functools

import jax
import jax.numpy as jnp
from jax import lax
from jax.experimental import pallas as pl
from jax.experimental.pallas import tpu as pltpu
from jax.sharding import PartitionSpec as P

TSN = 1501
SPECIALS = 108
INITIAL = 50

MASK_VALUE = -1000000000.0
EMPTY_VALUE = -3000000000.0
SLOPE = 4.0
FLOOR = -30.0


LANES = 128
FIELDS = 8
FAR = 1 << 30
GRANT = 24 << 20
NEAR = 4

DIRECT = (1,)


def source_of(piece, member, outer):
    if outer > NEAR:
        return piece
    step, side = piece % outer, piece // outer
    place = lax.rem(lax.div(member, 2) + step, outer)
    return 2 * place + (lax.rem(member, 2) ^ side)


def row_limits(prev_old, prev_new, last_stamp, sample_begin, seq_length, stamp_begin):
    generated = seq_length - sample_begin
    last_is = (generated >= 1) & (prev_new >= stamp_begin)
    before_is = (generated < 2) | (prev_old >= stamp_begin)
    both = last_is & before_is
    single = last_is & ~before_is
    begin = generated == 0
    text_low = jnp.where(begin, stamp_begin, jnp.where(single, stamp_begin - SPECIALS, 0))
    bound = stamp_begin + last_stamp + jnp.where(single, 0, 1)
    stamp_low = jnp.where(both, FAR, jnp.where(last_stamp >= 0, bound, stamp_begin))
    stamp_high = jnp.where(begin, stamp_begin + INITIAL + 1, FAR)
    return text_low, stamp_low, stamp_high


def prep_kernel(members, row_dev, stamp_begin, *refs):
    prev_in, stamp_in, begin_in, length_in, chosen_in, table, own = refs[:7]
    out, table_out, own_out = refs[7:10]
    prev, stamp, begin, length, chosen, sems = refs[10:]
    copies = [
        pltpu.make_async_copy(source, target, sems.at[i])
        for i, (source, target) in enumerate((
            (prev_in, prev), (stamp_in, stamp), (begin_in, begin), (length_in, length),
            (chosen_in, chosen), (own, own_out), (table, table_out),
        ))
    ]
    for copy in copies:
        copy.start()
    for copy in copies[:5]:
        copy.wait()
    index = lax.axis_index("vocab")
    per_tile = LANES // row_dev
    lane = lax.broadcasted_iota(jnp.int32, (FIELDS, LANES), 1)
    for tile in range(members // per_tile):
        total = jnp.zeros((FIELDS, LANES), jnp.int32)
        for place in range(per_tile):
            owner = source_of(tile * per_tile + place, lax.div(index, 2), members // 2)
            source = 2 * owner + lax.rem(index, 2)
            at = pl.multiple_of(lax.div(source, per_tile) * LANES, LANES)
            span = pl.ds(at, LANES)
            limits = row_limits(
                prev[0:1, span], prev[1:2, span], stamp[:, span], begin[:, span], length[:, span],
                stamp_begin,
            )
            fields = jnp.concatenate(list(limits) + [chosen[:, span]], axis=0)
            shift = lax.rem(place - lax.rem(source, per_tile) + per_tile, per_tile) * row_dev
            moved = pltpu.roll(fields, shift, 1)
            here = (lane >= place * row_dev) & (lane < (place + 1) * row_dev)
            total = jnp.where(here, moved, total)
        out[:, tile * LANES:(tile + 1) * LANES] = total
    for copy in copies[5:]:
        copy.wait()


def stats_kernel(members, row_dev, stamp_begin, *refs):
    *parts, table, other, limits, out = refs
    index = lax.axis_index("vocab")
    member = lax.div(index, 2)
    outer = members // 2
    width = table.shape[0]
    per_tile = LANES // row_dev
    if outer > NEAR:
        pieces = parts[0][...]
    else:
        pieces = jnp.concatenate([part[...] for part in parts], axis=0)
    for tile in range(members // per_tile):
        span = slice(tile * LANES, (tile + 1) * LANES)
        rows = pieces[span]
        lim = limits[:, span]
        text_low, stamp_low, stamp_high = lim[0:1], lim[1:2], lim[2:3]
        halves = []
        for ref, shard in ((table, index), (other, index ^ 1)):
            logits = lax.dot_general(
                ref[...], rows, (((1,), (1,)), ((), ())), preferred_element_type=jnp.float32
            )
            column = shard * width + lax.broadcasted_iota(jnp.int32, (width, LANES), 0)
            is_text = column < stamp_begin
            low = jnp.where(is_text, text_low, stamp_low)
            high = jnp.where(is_text, stamp_begin - 1, stamp_high)
            values = jnp.where((column >= low) & (column < high), logits, MASK_VALUE)
            halves.append((values, column, is_text))
        text_max = stamp_max = None
        for values, column, is_text in halves:
            text = jnp.max(jnp.where(is_text, values, EMPTY_VALUE), axis=0, keepdims=True)
            stamp = jnp.max(jnp.where(is_text, EMPTY_VALUE, values), axis=0, keepdims=True)
            text_max = text if text_max is None else jnp.maximum(text_max, text)
            stamp_max = stamp if stamp_max is None else jnp.maximum(stamp_max, stamp)
        text_total = jnp.zeros((1, LANES), jnp.float32)
        stamp_total = jnp.zeros((1, LANES), jnp.float32)
        picked = [jnp.zeros((1, LANES), jnp.float32) for _ in range(FIELDS - 3)]
        for values, column, is_text in halves:
            scaled = jnp.exp(values - jnp.where(is_text, text_max, stamp_max))
            text_total += jnp.sum(jnp.where(is_text, scaled, 0.0), axis=0, keepdims=True)
            stamp_total += jnp.sum(jnp.where(is_text, 0.0, scaled), axis=0, keepdims=True)
            for k in range(FIELDS - 3):
                hit = column == lim[3 + k:4 + k]
                picked[k] += jnp.sum(jnp.where(hit, values, 0.0), axis=0, keepdims=True)
        stats = [text_max, text_max + jnp.log(text_total), stamp_max + jnp.log(stamp_total)] + picked
        lane = lax.broadcasted_iota(jnp.int32, (per_tile, LANES), 1)
        packed = jnp.zeros((per_tile, LANES), jnp.float32)
        stacked = jnp.concatenate([stats[(-f) % FIELDS] for f in range(FIELDS)], axis=0)
        turned = pltpu.roll(stacked, 0, 1, stride=row_dev, stride_axis=0)
        for f in range(FIELDS):
            spread = jnp.broadcast_to(turned[f:f + 1], (per_tile, LANES))
            moved = pltpu.roll(spread, 0, 1, stride=row_dev, stride_axis=0)
            here = (lane >= f * row_dev) & (lane < (f + 1) * row_dev)
            packed = jnp.where(here, moved, packed)
        for place in range(per_tile):
            piece = tile * per_tile + (-place) % per_tile
            target = source_of(piece, member, members // 2)
            out[pl.ds(target, 1)] = packed[place:place + 1].reshape(1, 1, LANES)


def final_kernel(row_dev, stamp_begin, got, limits, picked_out, stamp_out):
    parts = got[:, 0, :]
    top = jnp.max(parts, axis=0, keepdims=True)
    lse = top + jnp.log(jnp.sum(jnp.exp(parts - top), axis=0, keepdims=True))
    total = jnp.sum(parts, axis=0, keepdims=True)
    lane = lax.broadcasted_iota(jnp.int32, (1, LANES), 1)
    lses = lane >= (FIELDS - 2) * row_dev
    merged = jnp.where(lane < row_dev, top, jnp.where(lses, lse, total))
    spread = jnp.broadcast_to(merged, (FIELDS, LANES))
    fields = pltpu.roll(spread, 0, 1, stride=row_dev, stride_axis=0)
    text_max, text_lse, stamp_lse = fields[0:1], fields[1:2], fields[2:3]
    penalty = SLOPE * jnp.maximum(stamp_lse - text_max, 0.0)
    shifted = text_lse - penalty
    larger = jnp.maximum(shifted, stamp_lse)
    total = larger + jnp.log(jnp.exp(shifted - larger) + jnp.exp(stamp_lse - larger))
    chosen = limits[:, 0:LANES]
    adjusted = fields - jnp.where(chosen < stamp_begin, penalty, 0.0) - total
    result = jnp.maximum(adjusted, FLOOR)
    picked_out[...] = result[3:, :row_dev]
    stamp_out[...] = jnp.maximum(stamp_lse - total, FLOOR)[:, :row_dev]


def per_device(hidden, embedding, prev_tokens, last_stamp, sample_begin, seq_length, chosen):
    width = embedding.shape[0]
    row_dev = hidden.shape[0]
    nsel = chosen.shape[0]
    count = lax.axis_size("vocab")
    members = count // 2
    outer = members // 2
    stamp_begin = width * count - TSN
    core_rows = members * row_dev

    def move(array, step, side):
        pairs = [(i, ((i - 4 * step) % count) ^ (2 * side)) for i in range(count)]
        return lax.ppermute(array, "vocab", pairs)

    if outer > NEAR:
        same = [[2 * i + core for i in range(members)] for core in range(2)]
        parts = [lax.all_gather(hidden, "vocab", axis_index_groups=same, tiled=True)]
    else:
        line, across = [hidden], [move(hidden, 0, 1)]
        for step in range(1, outer):
            line.append(move(hidden, step, 0))
            origin = (hidden, step) if step in DIRECT else (line[-1], 0)
            across.append(move(*origin, 1))
        parts = line + across
    other = lax.ppermute(embedding, "vocab", [(i, i ^ 1) for i in range(count)])
    state = (prev_tokens, last_stamp[None], sample_begin[None], seq_length[None], chosen)
    limits, table, own = pl.pallas_call(
        functools.partial(prep_kernel, members, row_dev, stamp_begin),
        in_specs=[pl.BlockSpec(memory_space=pltpu.HBM)] * 7,
        out_specs=[pl.BlockSpec(memory_space=pltpu.VMEM)] * 3,
        out_shape=(
            jax.ShapeDtypeStruct((FIELDS, core_rows), jnp.int32),
            jax.ShapeDtypeStruct(embedding.shape, embedding.dtype),
            jax.ShapeDtypeStruct(hidden.shape, hidden.dtype),
        ),
        scratch_shapes=[pltpu.VMEM(part.shape, part.dtype) for part in state]
        + [pltpu.SemaphoreType.DMA((7,))],
        name="prep",
        compiler_params=pltpu.CompilerParams(vmem_limit_bytes=GRANT),
    )(*(pltpu.with_memory_space_constraint(part, pltpu.HBM) for part in (*state, embedding, hidden)))
    if outer <= NEAR:
        parts[0] = own
    stats = pl.pallas_call(
        functools.partial(stats_kernel, members, row_dev, stamp_begin),
        out_shape=jax.ShapeDtypeStruct((members, 1, LANES), jnp.float32),
        name="stats",
        compiler_params=pltpu.CompilerParams(vmem_limit_bytes=GRANT),
    )(*parts, table, other, limits)
    same_core = [[2 * i + core for i in range(members)] for core in range(2)]
    got = lax.all_to_all(stats, "vocab", 0, 0, axis_index_groups=same_core, tiled=True)
    picked, stamped = pl.pallas_call(
        functools.partial(final_kernel, row_dev, stamp_begin),
        out_shape=(
            jax.ShapeDtypeStruct((nsel, row_dev), jnp.float32),
            jax.ShapeDtypeStruct((1, row_dev), jnp.float32),
        ),
        name="final",
        compiler_params=pltpu.CompilerParams(vmem_limit_bytes=GRANT),
    )(got, limits)
    return picked, stamped[0]


def solution(mesh):
    placed = (
        P(("groups", "vocab"), None),
        P("vocab", None),
        P(None, "groups"),
        P("groups"),
        P("groups"),
        P("groups"),
        P(None, "groups"),
    )
    return jax.shard_map(
        per_device,
        mesh=mesh,
        in_specs=placed,
        out_specs=(P(None, ("groups", "vocab")), P(("groups", "vocab"))),
        check_vma=False,
    )
```

```python
import functools

import jax
import jax.numpy as jnp
from jax import lax
from jax.experimental import pallas as pl
from jax.experimental.pallas import tpu as pltpu
from jax.sharding import PartitionSpec as P

TSN = 1501
SPECIALS = 108
INITIAL = 50

MASK_VALUE = -1000000000.0
EMPTY_VALUE = -3000000000.0
SLOPE = 4.0
FLOOR = -30.0


LANES = 128
SUBLANES = 8
FIELDS = 8
FAR = 1 << 30
GRANT = 24 << 20
NEAR = 4

DIRECT = (1,)


def source_of(piece, member, outer):
    if outer > NEAR:
        return piece
    step, side = piece % outer, piece // outer
    place = lax.rem(lax.div(member, 2) + step, outer)
    return 2 * place + (lax.rem(member, 2) ^ side)


def row_limits(prev_old, prev_new, last_stamp, sample_begin, seq_length, stamp_begin):
    generated = seq_length - sample_begin
    last_is = (generated >= 1) & (prev_new >= stamp_begin)
    before_is = (generated < 2) | (prev_old >= stamp_begin)
    both = last_is & before_is
    single = last_is & ~before_is
    begin = generated == 0
    text_low = jnp.where(begin, stamp_begin, jnp.where(single, stamp_begin - SPECIALS, 0))
    bound = stamp_begin + last_stamp + jnp.where(single, 0, 1)
    stamp_low = jnp.where(both, FAR, jnp.where(last_stamp >= 0, bound, stamp_begin))
    stamp_high = jnp.where(begin, stamp_begin + INITIAL + 1, FAR)
    return text_low, stamp_low, stamp_high


def prep_kernel(members, row_dev, stamp_begin, *refs):
    prev_in, stamp_in, begin_in, length_in, chosen_in, table, own = refs[:7]
    out, table_out, own_out = refs[7:10]
    prev, stamp, begin, length, chosen, sems = refs[10:]
    copies = [
        pltpu.make_async_copy(source, target, sems.at[i])
        for i, (source, target) in enumerate((
            (prev_in, prev), (stamp_in, stamp), (begin_in, begin), (length_in, length),
            (chosen_in, chosen), (own, own_out), (table, table_out),
        ))
    ]
    for copy in copies:
        copy.start()
    for copy in copies[:5]:
        copy.wait()
    index = lax.axis_index("vocab")
    per_tile = LANES // row_dev
    lane = lax.broadcasted_iota(jnp.int32, (FIELDS, LANES), 1)
    for tile in range(members // per_tile):
        total = jnp.zeros((FIELDS, LANES), jnp.int32)
        for place in range(per_tile):
            owner = source_of(tile * per_tile + place, lax.div(index, 2), members // 2)
            source = 2 * owner + lax.rem(index, 2)
            at = pl.multiple_of(lax.div(source, per_tile) * LANES, LANES)
            span = pl.ds(at, LANES)
            limits = row_limits(
                prev[0:1, span], prev[1:2, span], stamp[:, span], begin[:, span], length[:, span],
                stamp_begin,
            )
            fields = jnp.concatenate(list(limits) + [chosen[:, span]], axis=0)
            shift = lax.rem(place - lax.rem(source, per_tile) + per_tile, per_tile) * row_dev
            moved = pltpu.roll(fields, shift, 1)
            here = (lane >= place * row_dev) & (lane < (place + 1) * row_dev)
            total = jnp.where(here, moved, total)
        out[:, tile * LANES:(tile + 1) * LANES] = total
    for copy in copies[5:]:
        copy.wait()


def stats_kernel(members, row_dev, stamp_begin, *refs):
    *parts, table, other, limits, out = refs
    index = lax.axis_index("vocab")
    member = lax.div(index, 2)
    outer = members // 2
    width = table.shape[0]
    per_tile = LANES // row_dev
    home, edge = divmod(stamp_begin, width)
    edge_at = edge // SUBLANES * SUBLANES
    block = (SUBLANES, LANES)
    within = lax.broadcasted_iota(jnp.int32, block, 0)

    def wide(row):
        return jnp.broadcast_to(row, block)

    def tile_stats(rows, lim, tile):
        text_low, stamp_low, stamp_high = lim[0:1], lim[1:2], lim[2:3]
        picked = [jnp.zeros(block, jnp.float32) for _ in range(FIELDS - 3)]
        segments = []
        for ref, shard in ((table, index), (other, index ^ 1)):
            base = shard * width
            logits = lax.dot_general(
                ref[...], rows, (((1,), (1,)), ((), ())), preferred_element_type=jnp.float32
            )
            wanted = [wide(lim[3 + k:4 + k] - base) for k in range(FIELDS - 3)]
            for first, last in zip((0, edge_at, edge_at + SUBLANES), (edge_at, edge_at + SUBLANES, width)):
                if first == last:
                    continue
                if first == edge_at:
                    is_text = base + first + within < stamp_begin
                else:
                    is_text = wide(jnp.full((1, LANES), shard) < home + (1 if first < edge_at else 0))
                low = jnp.where(is_text, wide(text_low), wide(stamp_low)) - base
                high = jnp.where(is_text, stamp_begin - 1, wide(stamp_high)) - base
                values, top = [], None
                for at in range(first, last, SUBLANES):
                    column = within + at
                    open_here = (column >= low) & (column < high)
                    value = jnp.where(open_here, logits[at:at + SUBLANES], MASK_VALUE)
                    values.append(value)
                    top = value if top is None else jnp.maximum(top, value)
                    for k in range(FIELDS - 3):
                        picked[k] = jnp.where(column == wanted[k], value, picked[k])
                segments.append((is_text, values, top))
        text_top = stamp_top = jnp.full(block, EMPTY_VALUE)
        for is_text, _, top in segments:
            text_top = jnp.maximum(text_top, jnp.where(is_text, top, EMPTY_VALUE))
            stamp_top = jnp.maximum(stamp_top, jnp.where(is_text, EMPTY_VALUE, top))
        text_max = jnp.max(text_top, axis=0, keepdims=True)
        stamp_max = jnp.max(stamp_top, axis=0, keepdims=True)
        text_total = jnp.zeros(block, jnp.float32)
        stamp_total = jnp.zeros(block, jnp.float32)
        for is_text, values, _ in segments:
            top = jnp.where(is_text, wide(text_max), wide(stamp_max))
            total = jnp.zeros(block, jnp.float32)
            for value in values:
                total += jnp.exp(value - top)
            text_total += jnp.where(is_text, total, 0.0)
            stamp_total += jnp.where(is_text, 0.0, total)
        text_total = jnp.sum(text_total, axis=0, keepdims=True)
        stamp_total = jnp.sum(stamp_total, axis=0, keepdims=True)
        stats = [text_max, text_max + jnp.log(text_total), stamp_max + jnp.log(stamp_total)]
        stats += [jnp.sum(value, axis=0, keepdims=True) for value in picked]
        lane = lax.broadcasted_iota(jnp.int32, (per_tile, LANES), 1)
        packed = jnp.zeros((per_tile, LANES), jnp.float32)
        stacked = jnp.concatenate([stats[(-f) % FIELDS] for f in range(FIELDS)], axis=0)
        turned = pltpu.roll(stacked, 0, 1, stride=row_dev, stride_axis=0)
        for f in range(FIELDS):
            spread = jnp.broadcast_to(turned[f:f + 1], (per_tile, LANES))
            moved = pltpu.roll(spread, 0, 1, stride=row_dev, stride_axis=0)
            here = (lane >= f * row_dev) & (lane < (f + 1) * row_dev)
            packed = jnp.where(here, moved, packed)
        for place in range(per_tile):
            piece = tile * per_tile + (-place) % per_tile
            target = source_of(piece, member, outer)
            out[pl.ds(target, 1)] = packed[place:place + 1].reshape(1, 1, LANES)

    if outer > NEAR:
        @pl.loop(0, members // per_tile)
        def _(tile):
            span = pl.ds(pl.multiple_of(tile * LANES, LANES), LANES)
            tile_stats(parts[0][span, :], limits[:, span], tile)
    else:
        rows = jnp.concatenate([part[...] for part in parts], axis=0)
        for tile in range(members // per_tile):
            span = slice(tile * LANES, (tile + 1) * LANES)
            tile_stats(rows[span], limits[:, span], tile)


def final_kernel(row_dev, stamp_begin, got, limits, picked_out, stamp_out):
    parts = got[:, 0, :]
    top = jnp.max(parts, axis=0, keepdims=True)
    lse = top + jnp.log(jnp.sum(jnp.exp(parts - top), axis=0, keepdims=True))
    total = jnp.sum(parts, axis=0, keepdims=True)
    lane = lax.broadcasted_iota(jnp.int32, (1, LANES), 1)
    lses = lane >= (FIELDS - 2) * row_dev
    merged = jnp.where(lane < row_dev, top, jnp.where(lses, lse, total))
    spread = jnp.broadcast_to(merged, (FIELDS, LANES))
    fields = pltpu.roll(spread, 0, 1, stride=row_dev, stride_axis=0)
    text_max, text_lse, stamp_lse = fields[0:1], fields[1:2], fields[2:3]
    penalty = SLOPE * jnp.maximum(stamp_lse - text_max, 0.0)
    shifted = text_lse - penalty
    larger = jnp.maximum(shifted, stamp_lse)
    total = larger + jnp.log(jnp.exp(shifted - larger) + jnp.exp(stamp_lse - larger))
    chosen = limits[:, 0:LANES]
    adjusted = fields - jnp.where(chosen < stamp_begin, penalty, 0.0) - total
    result = jnp.maximum(adjusted, FLOOR)
    picked_out[...] = result[3:, :row_dev]
    stamp_out[...] = jnp.maximum(stamp_lse - total, FLOOR)[:, :row_dev]


def per_device(hidden, embedding, prev_tokens, last_stamp, sample_begin, seq_length, chosen):
    width = embedding.shape[0]
    row_dev = hidden.shape[0]
    nsel = chosen.shape[0]
    count = lax.axis_size("vocab")
    members = count // 2
    outer = members // 2
    stamp_begin = width * count - TSN
    core_rows = members * row_dev

    def move(array, step, side):
        pairs = [(i, ((i - 4 * step) % count) ^ (2 * side)) for i in range(count)]
        return lax.ppermute(array, "vocab", pairs)

    if outer > NEAR:
        same = [[2 * i + core for i in range(members)] for core in range(2)]
        parts = [lax.all_gather(hidden, "vocab", axis_index_groups=same, tiled=True)]
    else:
        line, across = [hidden], [move(hidden, 0, 1)]
        for step in range(1, outer):
            line.append(move(hidden, step, 0))
            origin = (hidden, step) if step in DIRECT else (line[-1], 0)
            across.append(move(*origin, 1))
        parts = line + across
    other = lax.ppermute(embedding, "vocab", [(i, i ^ 1) for i in range(count)])
    state = (prev_tokens, last_stamp[None], sample_begin[None], seq_length[None], chosen)
    limits, table, own = pl.pallas_call(
        functools.partial(prep_kernel, members, row_dev, stamp_begin),
        in_specs=[pl.BlockSpec(memory_space=pltpu.HBM)] * 7,
        out_specs=[pl.BlockSpec(memory_space=pltpu.VMEM)] * 3,
        out_shape=(
            jax.ShapeDtypeStruct((FIELDS, core_rows), jnp.int32),
            jax.ShapeDtypeStruct(embedding.shape, embedding.dtype),
            jax.ShapeDtypeStruct(hidden.shape, hidden.dtype),
        ),
        scratch_shapes=[pltpu.VMEM(part.shape, part.dtype) for part in state]
        + [pltpu.SemaphoreType.DMA((7,))],
        name="prep",
        compiler_params=pltpu.CompilerParams(vmem_limit_bytes=GRANT),
    )(*(pltpu.with_memory_space_constraint(part, pltpu.HBM) for part in (*state, embedding, hidden)))
    if outer <= NEAR:
        parts[0] = own
    stats = pl.pallas_call(
        functools.partial(stats_kernel, members, row_dev, stamp_begin),
        out_shape=jax.ShapeDtypeStruct((members, 1, LANES), jnp.float32),
        name="stats",
        compiler_params=pltpu.CompilerParams(vmem_limit_bytes=GRANT),
    )(*parts, table, other, limits)
    same_core = [[2 * i + core for i in range(members)] for core in range(2)]
    got = lax.all_to_all(stats, "vocab", 0, 0, axis_index_groups=same_core, tiled=True)
    picked, stamped = pl.pallas_call(
        functools.partial(final_kernel, row_dev, stamp_begin),
        out_shape=(
            jax.ShapeDtypeStruct((nsel, row_dev), jnp.float32),
            jax.ShapeDtypeStruct((1, row_dev), jnp.float32),
        ),
        name="final",
        compiler_params=pltpu.CompilerParams(vmem_limit_bytes=GRANT),
    )(got, limits)
    return picked, stamped[0]


def solution(mesh):
    placed = (
        P(("groups", "vocab"), None),
        P("vocab", None),
        P(None, "groups"),
        P("groups"),
        P("groups"),
        P("groups"),
        P(None, "groups"),
    )
    return jax.shard_map(
        per_device,
        mesh=mesh,
        in_specs=placed,
        out_specs=(P(None, ("groups", "vocab")), P(("groups", "vocab"))),
        check_vma=False,
    )
```

```python
import functools

import jax
import jax.numpy as jnp
from jax import lax
from jax.experimental import pallas as pl
from jax.experimental.pallas import tpu as pltpu
from jax.sharding import PartitionSpec as P

TSN = 1501
SPECIALS = 108
INITIAL = 50

MASK_VALUE = -1000000000.0
EMPTY_VALUE = -3000000000.0
SLOPE = 4.0
FLOOR = -30.0


LANES = 128
SUBLANES = 8
FIELDS = 8
FAR = 1 << 30
GRANT = 24 << 20
NEAR = 4

DIRECT = (1,)


def source_of(piece, member, outer):
    if outer > NEAR:
        return piece
    step, side = piece % outer, piece // outer
    place = lax.rem(lax.div(member, 2) + step, outer)
    return 2 * place + (lax.rem(member, 2) ^ side)


def row_limits(prev_old, prev_new, last_stamp, sample_begin, seq_length, stamp_begin):
    generated = seq_length - sample_begin
    last_is = (generated >= 1) & (prev_new >= stamp_begin)
    before_is = (generated < 2) | (prev_old >= stamp_begin)
    both = last_is & before_is
    single = last_is & ~before_is
    begin = generated == 0
    text_low = jnp.where(begin, stamp_begin, jnp.where(single, stamp_begin - SPECIALS, 0))
    bound = stamp_begin + last_stamp + jnp.where(single, 0, 1)
    stamp_low = jnp.where(both, FAR, jnp.where(last_stamp >= 0, bound, stamp_begin))
    stamp_high = jnp.where(begin, stamp_begin + INITIAL + 1, FAR)
    return text_low, stamp_low, stamp_high


def prep_kernel(members, row_dev, stamp_begin, *refs):
    prev_in, stamp_in, begin_in, length_in, chosen_in, table, own = refs[:7]
    out, table_out, own_out = refs[7:10]
    prev, stamp, begin, length, chosen, sems = refs[10:]
    copies = [
        pltpu.make_async_copy(source, target, sems.at[i])
        for i, (source, target) in enumerate((
            (prev_in, prev), (stamp_in, stamp), (begin_in, begin), (length_in, length),
            (chosen_in, chosen), (own, own_out), (table, table_out),
        ))
    ]
    for copy in copies:
        copy.start()
    for copy in copies[:5]:
        copy.wait()
    index = lax.axis_index("vocab")
    per_tile = LANES // row_dev
    lane = lax.broadcasted_iota(jnp.int32, (FIELDS, LANES), 1)
    for tile in range(members // per_tile):
        total = jnp.zeros((FIELDS, LANES), jnp.int32)
        for place in range(per_tile):
            owner = source_of(tile * per_tile + place, lax.div(index, 2), members // 2)
            source = 2 * owner + lax.rem(index, 2)
            at = pl.multiple_of(lax.div(source, per_tile) * LANES, LANES)
            span = pl.ds(at, LANES)
            limits = row_limits(
                prev[0:1, span], prev[1:2, span], stamp[:, span], begin[:, span], length[:, span],
                stamp_begin,
            )
            fields = jnp.concatenate(list(limits) + [chosen[:, span]], axis=0)
            shift = lax.rem(place - lax.rem(source, per_tile) + per_tile, per_tile) * row_dev
            moved = pltpu.roll(fields, shift, 1)
            here = (lane >= place * row_dev) & (lane < (place + 1) * row_dev)
            total = jnp.where(here, moved, total)
        out[:, tile * LANES:(tile + 1) * LANES] = total
    for copy in copies[5:]:
        copy.wait()


def stats_kernel(members, row_dev, stamp_begin, *refs):
    *parts, table, other, limits, out = refs
    index = lax.axis_index("vocab")
    member = lax.div(index, 2)
    outer = members // 2
    width = table.shape[0]
    per_tile = LANES // row_dev
    home, edge = divmod(stamp_begin, width)
    edge_at = edge // SUBLANES * SUBLANES
    block = (SUBLANES, LANES)
    within = lax.broadcasted_iota(jnp.int32, block, 0)

    def wide(row):
        return jnp.broadcast_to(row, block)

    def tile_stats(rows, lim, tile):
        text_low, stamp_low, stamp_high = lim[0:1], lim[1:2], lim[2:3]
        picked = [jnp.zeros(block, jnp.float32) for _ in range(FIELDS - 3)]
        segments = []
        both = lax.dot_general(
            jnp.concatenate([table[...], other[...]], axis=0), rows, (((1,), (1,)), ((), ())),
            preferred_element_type=jnp.float32,
        )
        for half, shard in enumerate((index, index ^ 1)):
            base = shard * width
            logits = both[half * width:(half + 1) * width]
            wanted = [wide(lim[3 + k:4 + k] - base) for k in range(FIELDS - 3)]
            for first, last in zip((0, edge_at, edge_at + SUBLANES), (edge_at, edge_at + SUBLANES, width)):
                if first == last:
                    continue
                if first == edge_at:
                    is_text = base + first + within < stamp_begin
                else:
                    is_text = wide(jnp.full((1, LANES), shard) < home + (1 if first < edge_at else 0))
                low = jnp.where(is_text, wide(text_low), wide(stamp_low)) - base
                high = jnp.where(is_text, stamp_begin - 1, wide(stamp_high)) - base
                values, top = [], None
                for at in range(first, last, SUBLANES):
                    column = within + at
                    open_here = (column >= low) & (column < high)
                    value = jnp.where(open_here, logits[at:at + SUBLANES], MASK_VALUE)
                    values.append(value)
                    top = value if top is None else jnp.maximum(top, value)
                    for k in range(FIELDS - 3):
                        picked[k] = jnp.where(column == wanted[k], value, picked[k])
                segments.append((is_text, values, top))
        text_top = stamp_top = jnp.full(block, EMPTY_VALUE)
        for is_text, _, top in segments:
            text_top = jnp.maximum(text_top, jnp.where(is_text, top, EMPTY_VALUE))
            stamp_top = jnp.maximum(stamp_top, jnp.where(is_text, EMPTY_VALUE, top))
        text_max = jnp.max(text_top, axis=0, keepdims=True)
        stamp_max = jnp.max(stamp_top, axis=0, keepdims=True)
        text_total = jnp.zeros(block, jnp.float32)
        stamp_total = jnp.zeros(block, jnp.float32)
        for is_text, values, _ in segments:
            top = jnp.where(is_text, wide(text_max), wide(stamp_max))
            total = jnp.zeros(block, jnp.float32)
            for value in values:
                total += jnp.exp(value - top)
            text_total += jnp.where(is_text, total, 0.0)
            stamp_total += jnp.where(is_text, 0.0, total)
        text_total = jnp.sum(text_total, axis=0, keepdims=True)
        stamp_total = jnp.sum(stamp_total, axis=0, keepdims=True)
        stats = [text_max, text_max + jnp.log(text_total), stamp_max + jnp.log(stamp_total)]
        stats += [jnp.sum(value, axis=0, keepdims=True) for value in picked]
        lane = lax.broadcasted_iota(jnp.int32, (per_tile, LANES), 1)
        packed = jnp.zeros((per_tile, LANES), jnp.float32)
        stacked = jnp.concatenate([stats[(-f) % FIELDS] for f in range(FIELDS)], axis=0)
        turned = pltpu.roll(stacked, 0, 1, stride=row_dev, stride_axis=0)
        for f in range(FIELDS):
            spread = jnp.broadcast_to(turned[f:f + 1], (per_tile, LANES))
            moved = pltpu.roll(spread, 0, 1, stride=row_dev, stride_axis=0)
            here = (lane >= f * row_dev) & (lane < (f + 1) * row_dev)
            packed = jnp.where(here, moved, packed)
        for place in range(per_tile):
            piece = tile * per_tile + (-place) % per_tile
            target = source_of(piece, member, outer)
            slot = lax.rem(target + members // 2, members)
            out[pl.ds(slot, 1)] = packed[place:place + 1].reshape(1, 1, LANES)

    if outer > NEAR:
        @pl.loop(0, members // per_tile)
        def _(tile):
            span = pl.ds(pl.multiple_of(tile * LANES, LANES), LANES)
            tile_stats(parts[0][span, :], limits[:, span], tile)
    else:
        rows = jnp.concatenate([part[...] for part in parts], axis=0)
        for tile in range(members // per_tile):
            span = slice(tile * LANES, (tile + 1) * LANES)
            tile_stats(rows[span], limits[:, span], tile)


def final_kernel(row_dev, stamp_begin, got, limits, picked_out, stamp_out):
    parts = got[:, 0, :]
    top = jnp.max(parts, axis=0, keepdims=True)
    lse = top + jnp.log(jnp.sum(jnp.exp(parts - top), axis=0, keepdims=True))
    total = jnp.sum(parts, axis=0, keepdims=True)
    lane = lax.broadcasted_iota(jnp.int32, (1, LANES), 1)
    lses = lane >= (FIELDS - 2) * row_dev
    merged = jnp.where(lane < row_dev, top, jnp.where(lses, lse, total))
    spread = jnp.broadcast_to(merged, (FIELDS, LANES))
    fields = pltpu.roll(spread, 0, 1, stride=row_dev, stride_axis=0)
    text_max, text_lse, stamp_lse = fields[0:1], fields[1:2], fields[2:3]
    penalty = SLOPE * jnp.maximum(stamp_lse - text_max, 0.0)
    shifted = text_lse - penalty
    larger = jnp.maximum(shifted, stamp_lse)
    total = larger + jnp.log(jnp.exp(shifted - larger) + jnp.exp(stamp_lse - larger))
    chosen = limits[:, 0:LANES]
    adjusted = fields - jnp.where(chosen < stamp_begin, penalty, 0.0) - total
    result = jnp.maximum(adjusted, FLOOR)
    picked_out[...] = result[3:, :row_dev]
    stamp_out[...] = jnp.maximum(stamp_lse - total, FLOOR)[:, :row_dev]


def per_device(hidden, embedding, prev_tokens, last_stamp, sample_begin, seq_length, chosen):
    width = embedding.shape[0]
    row_dev = hidden.shape[0]
    nsel = chosen.shape[0]
    count = lax.axis_size("vocab")
    members = count // 2
    outer = members // 2
    stamp_begin = width * count - TSN
    core_rows = members * row_dev

    def move(array, step, side):
        pairs = [(i, ((i - 4 * step) % count) ^ (2 * side)) for i in range(count)]
        return lax.ppermute(array, "vocab", pairs)

    if outer > NEAR:
        same = [[2 * i + core for i in range(members)] for core in range(2)]
        parts = [lax.all_gather(hidden, "vocab", axis_index_groups=same, tiled=True)]
    else:
        line, across = [hidden], [move(hidden, 0, 1)]
        for step in range(1, outer):
            line.append(move(hidden, step, 0))
            origin = (hidden, step) if step in DIRECT else (line[-1], 0)
            across.append(move(*origin, 1))
        parts = line + across
    other = lax.ppermute(embedding, "vocab", [(i, i ^ 1) for i in range(count)])
    state = (prev_tokens, last_stamp[None], sample_begin[None], seq_length[None], chosen)
    limits, table, own = pl.pallas_call(
        functools.partial(prep_kernel, members, row_dev, stamp_begin),
        in_specs=[pl.BlockSpec(memory_space=pltpu.HBM)] * 7,
        out_specs=[pl.BlockSpec(memory_space=pltpu.VMEM)] * 3,
        out_shape=(
            jax.ShapeDtypeStruct((FIELDS, core_rows), jnp.int32),
            jax.ShapeDtypeStruct(embedding.shape, embedding.dtype),
            jax.ShapeDtypeStruct(hidden.shape, hidden.dtype),
        ),
        scratch_shapes=[pltpu.VMEM(part.shape, part.dtype) for part in state]
        + [pltpu.SemaphoreType.DMA((7,))],
        name="prep",
        compiler_params=pltpu.CompilerParams(vmem_limit_bytes=GRANT),
    )(*(pltpu.with_memory_space_constraint(part, pltpu.HBM) for part in (*state, embedding, hidden)))
    if outer <= NEAR:
        parts[0] = own
    stats = pl.pallas_call(
        functools.partial(stats_kernel, members, row_dev, stamp_begin),
        out_shape=jax.ShapeDtypeStruct((members, 1, LANES), jnp.float32),
        name="stats",
        compiler_params=pltpu.CompilerParams(vmem_limit_bytes=GRANT),
    )(*parts, table, other, limits)
    order = [(i + members // 2) % members for i in range(members)]
    same_core = [[2 * i + core for i in order] for core in range(2)]
    got = lax.all_to_all(stats, "vocab", 0, 0, axis_index_groups=same_core, tiled=True)
    picked, stamped = pl.pallas_call(
        functools.partial(final_kernel, row_dev, stamp_begin),
        out_shape=(
            jax.ShapeDtypeStruct((nsel, row_dev), jnp.float32),
            jax.ShapeDtypeStruct((1, row_dev), jnp.float32),
        ),
        name="final",
        compiler_params=pltpu.CompilerParams(vmem_limit_bytes=GRANT),
    )(got, limits)
    return picked, stamped[0]


def solution(mesh):
    placed = (
        P(("groups", "vocab"), None),
        P("vocab", None),
        P(None, "groups"),
        P("groups"),
        P("groups"),
        P("groups"),
        P(None, "groups"),
    )
    return jax.shard_map(
        per_device,
        mesh=mesh,
        in_specs=placed,
        out_specs=(P(None, ("groups", "vocab")), P(("groups", "vocab"))),
        check_vma=False,
    )
```

```python
import functools

import jax
import jax.numpy as jnp
from jax import lax
from jax.experimental import pallas as pl
from jax.experimental.pallas import tpu as pltpu
from jax.sharding import PartitionSpec as P

TSN = 1501
SPECIALS = 108
INITIAL = 50

MASK_VALUE = -1000000000.0
EMPTY_VALUE = -3000000000.0
SLOPE = 4.0
FLOOR = -30.0


LANES = 128
SUBLANES = 8
FIELDS = 8
FAR = 1 << 30
GRANT = 24 << 20
NEAR = 4

DIRECT = (1,)


def source_of(piece, member, outer):
    if outer > NEAR:
        return piece
    step, side = piece % outer, piece // outer
    place = lax.rem(lax.div(member, 2) + step, outer)
    return 2 * place + (lax.rem(member, 2) ^ side)


def row_limits(prev_old, prev_new, last_stamp, sample_begin, seq_length, stamp_begin):
    generated = seq_length - sample_begin
    last_is = (generated >= 1) & (prev_new >= stamp_begin)
    before_is = (generated < 2) | (prev_old >= stamp_begin)
    both = last_is & before_is
    single = last_is & ~before_is
    begin = generated == 0
    text_low = jnp.where(begin, stamp_begin, jnp.where(single, stamp_begin - SPECIALS, 0))
    bound = stamp_begin + last_stamp + jnp.where(single, 0, 1)
    stamp_low = jnp.where(both, FAR, jnp.where(last_stamp >= 0, bound, stamp_begin))
    stamp_high = jnp.where(begin, stamp_begin + INITIAL + 1, FAR)
    return text_low, stamp_low, stamp_high


def prep_kernel(members, row_dev, stamp_begin, *refs):
    prev_in, stamp_in, begin_in, length_in, chosen_in, table, own = refs[:7]
    out, table_out, own_out = refs[7:10]
    prev, stamp, begin, length, chosen, sems = refs[10:]
    copies = [
        pltpu.make_async_copy(source, target, sems.at[i])
        for i, (source, target) in enumerate((
            (prev_in, prev), (stamp_in, stamp), (begin_in, begin), (length_in, length),
            (chosen_in, chosen), (own, own_out), (table, table_out),
        ))
    ]
    for copy in copies:
        copy.start()
    for copy in copies[:5]:
        copy.wait()
    index = lax.axis_index("vocab")
    per_tile = LANES // row_dev
    lane = lax.broadcasted_iota(jnp.int32, (FIELDS, LANES), 1)

    def moved(owner, place):
        source = 2 * owner + lax.rem(index, 2)
        at = pl.multiple_of(lax.div(source, per_tile) * LANES, LANES)
        span = pl.ds(at, LANES)
        limits = row_limits(
            prev[0:1, span], prev[1:2, span], stamp[:, span], begin[:, span], length[:, span],
            stamp_begin,
        )
        fields = jnp.concatenate(list(limits) + [chosen[:, span]], axis=0)
        shift = lax.rem(place - lax.rem(source, per_tile) + per_tile, per_tile) * row_dev
        return pltpu.roll(fields, shift, 1)

    member = lax.div(index, 2)
    for tile in range(members // per_tile):
        total = jnp.zeros((FIELDS, LANES), jnp.int32)
        for place in range(per_tile):
            here = (lane >= place * row_dev) & (lane < (place + 1) * row_dev)
            owner = source_of(tile * per_tile + place, member, members // 2)
            total = jnp.where(here, moved(owner, place), total)
        out[:, tile * LANES:(tile + 1) * LANES] = total
    if members // 2 > NEAR:
        out[:, members * row_dev:] = moved(member, 0)
    for copy in copies[5:]:
        copy.wait()


def stats_kernel(members, row_dev, stamp_begin, *refs):
    *parts, table, other, limits, out = refs
    index = lax.axis_index("vocab")
    member = lax.div(index, 2)
    outer = members // 2
    width = table.shape[0]
    per_tile = LANES // row_dev
    home, edge = divmod(stamp_begin, width)
    edge_at = edge // SUBLANES * SUBLANES
    block = (SUBLANES, LANES)
    within = lax.broadcasted_iota(jnp.int32, block, 0)

    def wide(row):
        return jnp.broadcast_to(row, block)

    def tile_stats(rows, lim, tile):
        text_low, stamp_low, stamp_high = lim[0:1], lim[1:2], lim[2:3]
        picked = [jnp.zeros(block, jnp.float32) for _ in range(FIELDS - 3)]
        segments = []
        both = lax.dot_general(
            jnp.concatenate([table[...], other[...]], axis=0), rows, (((1,), (1,)), ((), ())),
            preferred_element_type=jnp.float32,
        )
        for half, shard in enumerate((index, index ^ 1)):
            base = shard * width
            logits = both[half * width:(half + 1) * width]
            wanted = [wide(lim[3 + k:4 + k] - base) for k in range(FIELDS - 3)]
            for first, last in zip((0, edge_at, edge_at + SUBLANES), (edge_at, edge_at + SUBLANES, width)):
                if first == last:
                    continue
                if first == edge_at:
                    is_text = base + first + within < stamp_begin
                else:
                    is_text = wide(jnp.full((1, LANES), shard) < home + (1 if first < edge_at else 0))
                low = jnp.where(is_text, wide(text_low), wide(stamp_low)) - base
                high = jnp.where(is_text, stamp_begin - 1, wide(stamp_high)) - base
                values, top = [], None
                for at in range(first, last, SUBLANES):
                    column = within + at
                    open_here = (column >= low) & (column < high)
                    value = jnp.where(open_here, logits[at:at + SUBLANES], MASK_VALUE)
                    values.append(value)
                    top = value if top is None else jnp.maximum(top, value)
                    for k in range(FIELDS - 3):
                        picked[k] = jnp.where(column == wanted[k], value, picked[k])
                segments.append((is_text, values, top))
        text_top = stamp_top = jnp.full(block, EMPTY_VALUE)
        for is_text, _, top in segments:
            text_top = jnp.maximum(text_top, jnp.where(is_text, top, EMPTY_VALUE))
            stamp_top = jnp.maximum(stamp_top, jnp.where(is_text, EMPTY_VALUE, top))
        text_max = jnp.max(text_top, axis=0, keepdims=True)
        stamp_max = jnp.max(stamp_top, axis=0, keepdims=True)
        text_total = jnp.zeros(block, jnp.float32)
        stamp_total = jnp.zeros(block, jnp.float32)
        for is_text, values, _ in segments:
            top = jnp.where(is_text, wide(text_max), wide(stamp_max))
            total = jnp.zeros(block, jnp.float32)
            for value in values:
                total += jnp.exp(value - top)
            text_total += jnp.where(is_text, total, 0.0)
            stamp_total += jnp.where(is_text, 0.0, total)
        text_total = jnp.sum(text_total, axis=0, keepdims=True)
        stamp_total = jnp.sum(stamp_total, axis=0, keepdims=True)
        stats = [text_max, text_max + jnp.log(text_total), stamp_max + jnp.log(stamp_total)]
        stats += [jnp.sum(value, axis=0, keepdims=True) for value in picked]
        lane = lax.broadcasted_iota(jnp.int32, (per_tile, LANES), 1)
        packed = jnp.zeros((per_tile, LANES), jnp.float32)
        stacked = jnp.concatenate([stats[(-f) % FIELDS] for f in range(FIELDS)], axis=0)
        turned = pltpu.roll(stacked, 0, 1, stride=row_dev, stride_axis=0)
        for f in range(FIELDS):
            spread = jnp.broadcast_to(turned[f:f + 1], (per_tile, LANES))
            moved = pltpu.roll(spread, 0, 1, stride=row_dev, stride_axis=0)
            here = (lane >= f * row_dev) & (lane < (f + 1) * row_dev)
            packed = jnp.where(here, moved, packed)
        for place in range(per_tile):
            piece = tile * per_tile + (-place) % per_tile
            target = source_of(piece, member, outer)
            slot = lax.rem(target + members // 2, members)
            out[pl.ds(slot, 1)] = packed[place:place + 1].reshape(1, 1, LANES)

    if outer > NEAR:
        @pl.loop(0, members // per_tile)
        def _(tile):
            span = pl.ds(pl.multiple_of(tile * LANES, LANES), LANES)
            tile_stats(parts[0][span, :], limits[:, span], tile)
    else:
        rows = jnp.concatenate([part[...] for part in parts], axis=0)
        for tile in range(members // per_tile):
            span = slice(tile * LANES, (tile + 1) * LANES)
            tile_stats(rows[span], limits[:, span], tile)


def final_kernel(row_dev, stamp_begin, own_at, got, limits, picked_out, stamp_out):
    parts = got[:, 0, :]
    top = jnp.max(parts, axis=0, keepdims=True)
    lse = top + jnp.log(jnp.sum(jnp.exp(parts - top), axis=0, keepdims=True))
    total = jnp.sum(parts, axis=0, keepdims=True)
    lane = lax.broadcasted_iota(jnp.int32, (1, LANES), 1)
    lses = lane >= (FIELDS - 2) * row_dev
    merged = jnp.where(lane < row_dev, top, jnp.where(lses, lse, total))
    spread = jnp.broadcast_to(merged, (FIELDS, LANES))
    fields = pltpu.roll(spread, 0, 1, stride=row_dev, stride_axis=0)
    text_max, text_lse, stamp_lse = fields[0:1], fields[1:2], fields[2:3]
    penalty = SLOPE * jnp.maximum(stamp_lse - text_max, 0.0)
    shifted = text_lse - penalty
    larger = jnp.maximum(shifted, stamp_lse)
    total = larger + jnp.log(jnp.exp(shifted - larger) + jnp.exp(stamp_lse - larger))
    chosen = limits[:, own_at:own_at + LANES]
    adjusted = fields - jnp.where(chosen < stamp_begin, penalty, 0.0) - total
    result = jnp.maximum(adjusted, FLOOR)
    picked_out[...] = result[3:, :row_dev]
    stamp_out[...] = jnp.maximum(stamp_lse - total, FLOOR)[:, :row_dev]


def per_device(hidden, embedding, prev_tokens, last_stamp, sample_begin, seq_length, chosen):
    width = embedding.shape[0]
    row_dev = hidden.shape[0]
    nsel = chosen.shape[0]
    count = lax.axis_size("vocab")
    members = count // 2
    outer = members // 2
    stamp_begin = width * count - TSN
    core_rows = members * row_dev
    own_at = core_rows if outer > NEAR else 0

    def move(array, step, side):
        pairs = [(i, ((i - 4 * step) % count) ^ (2 * side)) for i in range(count)]
        return lax.ppermute(array, "vocab", pairs)

    if outer > NEAR:
        same = [[2 * i + core for i in range(members)] for core in range(2)]
        parts = [lax.all_gather(hidden, "vocab", axis_index_groups=same, tiled=True)]
    else:
        line, across = [hidden], [move(hidden, 0, 1)]
        for step in range(1, outer):
            line.append(move(hidden, step, 0))
            origin = (hidden, step) if step in DIRECT else (line[-1], 0)
            across.append(move(*origin, 1))
        parts = line + across
    other = lax.ppermute(embedding, "vocab", [(i, i ^ 1) for i in range(count)])
    state = (prev_tokens, last_stamp[None], sample_begin[None], seq_length[None], chosen)
    limits, table, own = pl.pallas_call(
        functools.partial(prep_kernel, members, row_dev, stamp_begin),
        in_specs=[pl.BlockSpec(memory_space=pltpu.HBM)] * 7,
        out_specs=[pl.BlockSpec(memory_space=pltpu.VMEM)] * 3,
        out_shape=(
            jax.ShapeDtypeStruct((FIELDS, max(core_rows, own_at + LANES)), jnp.int32),
            jax.ShapeDtypeStruct(embedding.shape, embedding.dtype),
            jax.ShapeDtypeStruct(hidden.shape, hidden.dtype),
        ),
        scratch_shapes=[pltpu.VMEM(part.shape, part.dtype) for part in state]
        + [pltpu.SemaphoreType.DMA((7,))],
        name="prep",
        compiler_params=pltpu.CompilerParams(vmem_limit_bytes=GRANT),
    )(*(pltpu.with_memory_space_constraint(part, pltpu.HBM) for part in (*state, embedding, hidden)))
    if outer <= NEAR:
        parts[0] = own
    stats = pl.pallas_call(
        functools.partial(stats_kernel, members, row_dev, stamp_begin),
        out_shape=jax.ShapeDtypeStruct((members, 1, LANES), jnp.float32),
        name="stats",
        compiler_params=pltpu.CompilerParams(vmem_limit_bytes=GRANT),
    )(*parts, table, other, limits)
    order = [(i + members // 2) % members for i in range(members)]
    same_core = [[2 * i + core for i in order] for core in range(2)]
    got = lax.all_to_all(stats, "vocab", 0, 0, axis_index_groups=same_core, tiled=True)
    picked, stamped = pl.pallas_call(
        functools.partial(final_kernel, row_dev, stamp_begin, own_at),
        out_shape=(
            jax.ShapeDtypeStruct((nsel, row_dev), jnp.float32),
            jax.ShapeDtypeStruct((1, row_dev), jnp.float32),
        ),
        name="final",
        compiler_params=pltpu.CompilerParams(vmem_limit_bytes=GRANT),
    )(got, limits)
    return picked, stamped[0]


def solution(mesh):
    placed = (
        P(("groups", "vocab"), None),
        P("vocab", None),
        P(None, "groups"),
        P("groups"),
        P("groups"),
        P("groups"),
        P(None, "groups"),
    )
    return jax.shard_map(
        per_device,
        mesh=mesh,
        in_specs=placed,
        out_specs=(P(None, ("groups", "vocab")), P(("groups", "vocab"))),
        check_vma=False,
    )
```

```python
import functools

import jax
import jax.numpy as jnp
from jax import lax
from jax.experimental import pallas as pl
from jax.experimental.pallas import tpu as pltpu
from jax.sharding import PartitionSpec as P

TSN = 1501
SPECIALS = 108
INITIAL = 50

MASK_VALUE = -1000000000.0
EMPTY_VALUE = -3000000000.0
SLOPE = 4.0
FLOOR = -30.0


LANES = 128
SUBLANES = 8
FIELDS = 8
FAR = 1 << 30
GRANT = 24 << 20
NEAR = 4

DIRECT = 1


def source_of(piece, member, outer):
    if outer > NEAR:
        return piece
    step, side = piece % outer, piece // outer
    place = lax.rem(lax.div(member, 2) + step, outer)
    return 2 * place + (lax.rem(member, 2) ^ side)


def row_limits(prev_old, prev_new, last_stamp, sample_begin, seq_length, stamp_begin):
    generated = seq_length - sample_begin
    last_is = (generated >= 1) & (prev_new >= stamp_begin)
    before_is = (generated < 2) | (prev_old >= stamp_begin)
    both = last_is & before_is
    single = last_is & ~before_is
    begin = generated == 0
    text_low = jnp.where(begin, stamp_begin, jnp.where(single, stamp_begin - SPECIALS, 0))
    bound = stamp_begin + last_stamp + jnp.where(single, 0, 1)
    stamp_low = jnp.where(both, FAR, jnp.where(last_stamp >= 0, bound, stamp_begin))
    stamp_high = jnp.where(begin, stamp_begin + INITIAL + 1, FAR)
    return text_low, stamp_low, stamp_high


def prep_kernel(members, row_dev, stamp_begin, *refs):
    prev_in, stamp_in, begin_in, length_in, chosen_in, table, own = refs[:7]
    out, table_out, own_out = refs[7:10]
    prev, stamp, begin, length, chosen, sems = refs[10:]
    copies = [
        pltpu.make_async_copy(source, target, sems.at[i])
        for i, (source, target) in enumerate((
            (prev_in, prev), (stamp_in, stamp), (begin_in, begin), (length_in, length),
            (chosen_in, chosen), (own, own_out), (table, table_out),
        ))
    ]
    for copy in copies:
        copy.start()
    for copy in copies[:5]:
        copy.wait()
    index = lax.axis_index("vocab")
    per_tile = LANES // row_dev
    lane = lax.broadcasted_iota(jnp.int32, (FIELDS, LANES), 1)

    def moved(owner, place):
        source = 2 * owner + lax.rem(index, 2)
        at = pl.multiple_of(lax.div(source, per_tile) * LANES, LANES)
        span = pl.ds(at, LANES)
        limits = row_limits(
            prev[0:1, span], prev[1:2, span], stamp[:, span], begin[:, span], length[:, span],
            stamp_begin,
        )
        fields = jnp.concatenate(list(limits) + [chosen[:, span]], axis=0)
        shift = lax.rem(place - lax.rem(source, per_tile) + per_tile, per_tile) * row_dev
        return pltpu.roll(fields, shift, 1)

    member = lax.div(index, 2)
    for tile in range(members // per_tile):
        total = jnp.zeros((FIELDS, LANES), jnp.int32)
        for place in range(per_tile):
            here = (lane >= place * row_dev) & (lane < (place + 1) * row_dev)
            owner = source_of(tile * per_tile + place, member, members // 2)
            total = jnp.where(here, moved(owner, place), total)
        out[:, tile * LANES:(tile + 1) * LANES] = total
    if members // 2 > NEAR:
        out[:, members * row_dev:] = moved(member, 0)
    for copy in copies[5:]:
        copy.wait()


def stats_kernel(members, row_dev, stamp_begin, *refs):
    *parts, table, other, limits, out = refs
    index = lax.axis_index("vocab")
    member = lax.div(index, 2)
    outer = members // 2
    width = table.shape[0]
    per_tile = LANES // row_dev
    home, edge = divmod(stamp_begin, width)
    edge_at = edge // SUBLANES * SUBLANES
    block = (SUBLANES, LANES)
    within = lax.broadcasted_iota(jnp.int32, block, 0)

    def wide(row):
        return jnp.broadcast_to(row, block)

    def tile_stats(rows, lim, tile):
        text_low, stamp_low, stamp_high = lim[0:1], lim[1:2], lim[2:3]
        picked = [jnp.zeros(block, jnp.float32) for _ in range(FIELDS - 3)]
        segments = []
        both = lax.dot_general(
            jnp.concatenate([table[...], other[...]], axis=0), rows, (((1,), (1,)), ((), ())),
            preferred_element_type=jnp.float32,
        )
        for half, shard in enumerate((index, index ^ 1)):
            base = shard * width
            logits = both[half * width:(half + 1) * width]
            wanted = [wide(lim[3 + k:4 + k] - base) for k in range(FIELDS - 3)]
            for first, last in zip((0, edge_at, edge_at + SUBLANES), (edge_at, edge_at + SUBLANES, width)):
                if first == last:
                    continue
                if first == edge_at:
                    is_text = base + first + within < stamp_begin
                else:
                    is_text = wide(jnp.full((1, LANES), shard) < home + (1 if first < edge_at else 0))
                low = jnp.where(is_text, wide(text_low), wide(stamp_low)) - base
                high = jnp.where(is_text, stamp_begin - 1, wide(stamp_high)) - base
                values, top = [], None
                for at in range(first, last, SUBLANES):
                    column = within + at
                    open_here = (column >= low) & (column < high)
                    value = jnp.where(open_here, logits[at:at + SUBLANES], MASK_VALUE)
                    values.append(value)
                    top = value if top is None else jnp.maximum(top, value)
                    for k in range(FIELDS - 3):
                        picked[k] = jnp.where(column == wanted[k], value, picked[k])
                segments.append((is_text, values, top))
        text_top = stamp_top = jnp.full(block, EMPTY_VALUE)
        for is_text, _, top in segments:
            text_top = jnp.maximum(text_top, jnp.where(is_text, top, EMPTY_VALUE))
            stamp_top = jnp.maximum(stamp_top, jnp.where(is_text, EMPTY_VALUE, top))
        text_max = jnp.max(text_top, axis=0, keepdims=True)
        stamp_max = jnp.max(stamp_top, axis=0, keepdims=True)
        text_total = jnp.zeros(block, jnp.float32)
        stamp_total = jnp.zeros(block, jnp.float32)
        for is_text, values, _ in segments:
            top = jnp.where(is_text, wide(text_max), wide(stamp_max))
            total = jnp.zeros(block, jnp.float32)
            for value in values:
                total += jnp.exp(value - top)
            text_total += jnp.where(is_text, total, 0.0)
            stamp_total += jnp.where(is_text, 0.0, total)
        text_total = jnp.sum(text_total, axis=0, keepdims=True)
        stamp_total = jnp.sum(stamp_total, axis=0, keepdims=True)
        stats = [text_max, text_max + jnp.log(text_total), stamp_max + jnp.log(stamp_total)]
        stats += [jnp.sum(value, axis=0, keepdims=True) for value in picked]
        lane = lax.broadcasted_iota(jnp.int32, (per_tile, LANES), 1)
        packed = jnp.zeros((per_tile, LANES), jnp.float32)
        stacked = jnp.concatenate([stats[(-f) % FIELDS] for f in range(FIELDS)], axis=0)
        turned = pltpu.roll(stacked, 0, 1, stride=row_dev, stride_axis=0)
        for f in range(FIELDS):
            spread = jnp.broadcast_to(turned[f:f + 1], (per_tile, LANES))
            moved = pltpu.roll(spread, 0, 1, stride=row_dev, stride_axis=0)
            here = (lane >= f * row_dev) & (lane < (f + 1) * row_dev)
            packed = jnp.where(here, moved, packed)
        for place in range(per_tile):
            piece = tile * per_tile + (-place) % per_tile
            target = source_of(piece, member, outer)
            slot = lax.rem(target + members - 3 * members // 4, members)
            out[pl.ds(slot, 1)] = packed[place:place + 1].reshape(1, 1, LANES)

    if outer > NEAR:
        @pl.loop(0, members // per_tile)
        def _(tile):
            span = pl.ds(pl.multiple_of(tile * LANES, LANES), LANES)
            tile_stats(parts[0][span, :], limits[:, span], tile)
    else:
        rows = jnp.concatenate([part[...] for part in parts], axis=0)
        for tile in range(members // per_tile):
            span = slice(tile * LANES, (tile + 1) * LANES)
            tile_stats(rows[span], limits[:, span], tile)


def final_kernel(row_dev, stamp_begin, own_at, got, limits, picked_out, stamp_out):
    parts = got[:, 0, :]
    top = jnp.max(parts, axis=0, keepdims=True)
    lse = top + jnp.log(jnp.sum(jnp.exp(parts - top), axis=0, keepdims=True))
    total = jnp.sum(parts, axis=0, keepdims=True)
    lane = lax.broadcasted_iota(jnp.int32, (1, LANES), 1)
    lses = lane >= (FIELDS - 2) * row_dev
    merged = jnp.where(lane < row_dev, top, jnp.where(lses, lse, total))
    spread = jnp.broadcast_to(merged, (FIELDS, LANES))
    fields = pltpu.roll(spread, 0, 1, stride=row_dev, stride_axis=0)
    text_max, text_lse, stamp_lse = fields[0:1], fields[1:2], fields[2:3]
    penalty = SLOPE * jnp.maximum(stamp_lse - text_max, 0.0)
    shifted = text_lse - penalty
    larger = jnp.maximum(shifted, stamp_lse)
    total = larger + jnp.log(jnp.exp(shifted - larger) + jnp.exp(stamp_lse - larger))
    chosen = limits[:, own_at:own_at + LANES]
    adjusted = fields - jnp.where(chosen < stamp_begin, penalty, 0.0) - total
    result = jnp.maximum(adjusted, FLOOR)
    picked_out[...] = result[3:, :row_dev]
    stamp_out[...] = jnp.maximum(stamp_lse - total, FLOOR)[:, :row_dev]


def per_device(hidden, embedding, prev_tokens, last_stamp, sample_begin, seq_length, chosen):
    width = embedding.shape[0]
    row_dev = hidden.shape[0]
    nsel = chosen.shape[0]
    count = lax.axis_size("vocab")
    members = count // 2
    outer = members // 2
    stamp_begin = width * count - TSN
    core_rows = members * row_dev
    own_at = core_rows if outer > NEAR else 0

    def move(array, step, side):
        pairs = [(i, ((i - 4 * step) % count) ^ (2 * side)) for i in range(count)]
        return lax.ppermute(array, "vocab", pairs)

    if outer > NEAR:
        same = [[2 * i + core for i in range(members)] for core in range(2)]
        parts = [lax.all_gather(hidden, "vocab", axis_index_groups=same, tiled=True)]
    else:
        line = [hidden] + [move(hidden, step, 0) for step in range(1, outer)]
        across = [move(hidden, 0, 1)]
        across += [move(hidden, step, 1) for step in range(1, min(outer, DIRECT + 1))]
        if len(line) > len(across):
            across.append(move(jnp.concatenate(line[len(across):], axis=0), 0, 1))
        parts = line + across
    other = lax.ppermute(embedding, "vocab", [(i, i ^ 1) for i in range(count)])
    state = (prev_tokens, last_stamp[None], sample_begin[None], seq_length[None], chosen)
    limits, table, own = pl.pallas_call(
        functools.partial(prep_kernel, members, row_dev, stamp_begin),
        in_specs=[pl.BlockSpec(memory_space=pltpu.HBM)] * 7,
        out_specs=[pl.BlockSpec(memory_space=pltpu.VMEM)] * 3,
        out_shape=(
            jax.ShapeDtypeStruct((FIELDS, max(core_rows, own_at + LANES)), jnp.int32),
            jax.ShapeDtypeStruct(embedding.shape, embedding.dtype),
            jax.ShapeDtypeStruct(hidden.shape, hidden.dtype),
        ),
        scratch_shapes=[pltpu.VMEM(part.shape, part.dtype) for part in state]
        + [pltpu.SemaphoreType.DMA((7,))],
        name="prep",
        compiler_params=pltpu.CompilerParams(vmem_limit_bytes=GRANT),
    )(*(pltpu.with_memory_space_constraint(part, pltpu.HBM) for part in (*state, embedding, hidden)))
    if outer <= NEAR:
        parts[0] = own
    stats = pl.pallas_call(
        functools.partial(stats_kernel, members, row_dev, stamp_begin),
        out_shape=jax.ShapeDtypeStruct((members, 1, LANES), jnp.float32),
        name="stats",
        compiler_params=pltpu.CompilerParams(vmem_limit_bytes=GRANT),
    )(*parts, table, other, limits)
    order = [(i + 3 * members // 4) % members for i in range(members)]
    same_core = [[2 * i + core for i in order] for core in range(2)]
    got = lax.all_to_all(stats, "vocab", 0, 0, axis_index_groups=same_core, tiled=True)
    picked, stamped = pl.pallas_call(
        functools.partial(final_kernel, row_dev, stamp_begin, own_at),
        out_shape=(
            jax.ShapeDtypeStruct((nsel, row_dev), jnp.float32),
            jax.ShapeDtypeStruct((1, row_dev), jnp.float32),
        ),
        name="final",
        compiler_params=pltpu.CompilerParams(vmem_limit_bytes=GRANT),
    )(got, limits)
    return picked, stamped[0]


def solution(mesh):
    placed = (
        P(("groups", "vocab"), None),
        P("vocab", None),
        P(None, "groups"),
        P("groups"),
        P("groups"),
        P("groups"),
        P(None, "groups"),
    )
    return jax.shard_map(
        per_device,
        mesh=mesh,
        in_specs=placed,
        out_specs=(P(None, ("groups", "vocab")), P(("groups", "vocab"))),
        check_vma=False,
    )
```
